32 devices in a mesh: tp: 8 (over z, y), dp: 4 (over x, core).
Axes of the slice: x: 2, y: 2, z: 4, core: 2. Of those that a mesh axis runs over, the one named last changes fastest.
Arguments:
- tokens: bfloat16 [768, 4096], P(('dp', 'tp')), may hold values from -6 to 6
- hidden_grad: bfloat16 [768, 14336], P('dp', 'tp'), may hold values from -0.59765625 to 0.59765625
- gate_value: bfloat16 [768, 14336], P('dp', 'tp'), may hold values from -6 to 6
- up_value: bfloat16 [768, 14336], P('dp', 'tp'), may hold values from -6 to 6
- gate_weight: bfloat16 [4096, 14336], P('dp', 'tp'), may hold values from -0.09375 to 0.09375
- up_weight: bfloat16 [4096, 14336], P('dp', 'tp'), may hold values from -0.09375 to 0.09375
Outputs:
- input_grad: bfloat16 [768, 4096], P(('dp', 'tp'))
- gate_grad: bfloat16 [4096, 14336], P('dp', 'tp')
- up_grad: bfloat16 [4096, 14336], P('dp', 'tp')
The draws below stay inside these ranges and needn't reach their ends.
All inputs are finite; a program needn't handle non-finite values.
Results may differ from the reference program's by a relative error of at most 0.018.
Values may be sent and summed in bfloat16 or wider, within the bound.
A program may use at most 128 MiB of HBM per device.

```python
import jax
import jax.numpy as jnp
from jax import lax

D = 4096
FF = 14336
TOK_DEV = 24
TOKENS = 768
N_TP = 8
N_DP = 4


def spiked(drawn, key, source, target, shards_of, factor):
    owner, partner = [(jnp.arange(drawn.shape[axis_at]) // (drawn.shape[axis_at] // shards_of)).reshape([-1 if axis == axis_at else 1 for axis in range(drawn.ndim)]) for axis_at in (source, target)]
    chosen = jax.random.permutation(key, shards_of)[partner]
    strong = (owner == chosen) | (owner == (partner + shards_of // 2) % shards_of)
    return jnp.where(strong, factor * drawn, drawn)


def block_levels(own_key, shape, pieces, least, high):
    factor_of = 1.0
    for axis_at, shards_of in pieces:
        heights = jax.random.uniform(jax.random.fold_in(jax.random.fold_in(own_key, 6), axis_at), (shards_of,), jnp.float32, least / len(pieces), high / len(pieces))
        factor_of = factor_of * jnp.repeat(jnp.exp(heights), shape[axis_at] // shards_of).reshape((-1,) + (1,) * (len(shape) - 1 - axis_at))
    return factor_of


def normal_values(key, extent, deviation, bound, shards=(), held_as=jnp.bfloat16):
    entries = deviation * jax.random.normal(key, extent, jnp.float32)
    if shards:
        entries = entries * block_levels(key, extent, shards, -0.22, 0.18)
    return jnp.clip(entries, -bound, bound).astype(held_as)


def noise_with(key, extent, scale, reach, pieces, heavy, held_as=jnp.bfloat16):
    array = scale * jax.random.normal(key, extent, jnp.float32)
    if pieces:
        array = array * block_levels(key, extent, pieces, -0.22, 0.18)
    return jnp.clip(spiked(array, jax.random.fold_in(key, 3), *heavy), -reach, reach).astype(held_as)


def setup_inputs(seed: int = 0) -> dict:
    keys = jax.random.split(jax.random.key(seed), 7)
    tokens = noise_with(keys[0], (TOKENS, D), 1.0, 6.0, ((0, 32),), (0, 1, 32, 2.75))
    hidden_grad = normal_values(keys[1], (TOKENS, FF), 0.1, 0.59765625, ((0, 4), (1, 8)))
    gate_value = normal_values(keys[2], (TOKENS, FF), 1.0, 6.0, ((0, 4), (1, 8)))
    up_value = normal_values(keys[3], (TOKENS, FF), 1.0, 6.0, ((0, 4), (1, 8)))
    gate_weight = normal_values(keys[4], (D, FF), D ** -0.5, 0.09375, ((0, 4), (1, 8)))
    up_weight = normal_values(keys[5], (D, FF), D ** -0.5, 0.09375, ((0, 4), (1, 8)))
    return dict(tokens=tokens, hidden_grad=hidden_grad, gate_value=gate_value, up_value=up_value, gate_weight=gate_weight, up_weight=up_weight)


def reference(tokens, hidden_grad, gate_value, up_value, gate_weight, up_weight):
    gate_float = gate_value.astype(jnp.float32)
    up_float = up_value.astype(jnp.float32)
    logistic = jax.nn.sigmoid(gate_float)
    upstream = hidden_grad.astype(jnp.float32)
    d_gate = (upstream * up_float * logistic * (1.0 + gate_float * (1.0 - logistic))).astype(jnp.bfloat16)
    d_up = (upstream * gate_float * logistic).astype(jnp.bfloat16)
    input_grad = (jnp.dot(d_gate, gate_weight.T, preferred_element_type=jnp.float32)
                  + jnp.dot(d_up, up_weight.T, preferred_element_type=jnp.float32)).astype(jnp.bfloat16)
    group_rows = TOK_DEV * N_TP
    contract = (((0,), (0,)), ((), ()))

    def per_group(carried, group_index):
        first_row = (group_index * group_rows).astype(jnp.int32)
        block = lax.dynamic_slice_in_dim(tokens, first_row, group_rows, 0)
        gate_rows = lax.dynamic_slice_in_dim(d_gate, first_row, group_rows, 0)
        up_rows = lax.dynamic_slice_in_dim(d_up, first_row, group_rows, 0)
        gate_part = lax.dot_general(block, gate_rows, contract, preferred_element_type=jnp.float32).astype(jnp.bfloat16)
        up_part = lax.dot_general(block, up_rows, contract, preferred_element_type=jnp.float32).astype(jnp.bfloat16)
        gate_part, up_part = lax.optimization_barrier((gate_part, up_part))
        return (carried[0] + gate_part.astype(jnp.float32), carried[1] + up_part.astype(jnp.float32)), None

    empty = jnp.zeros((D, FF), jnp.float32)
    summed, unused = lax.scan(per_group, (empty, empty), jnp.arange(N_DP, dtype=jnp.int32))
    return input_grad, summed[0].astype(jnp.bfloat16), summed[1].astype(jnp.bfloat16)
```

```python
import jax
import jax.numpy as jnp
from jax import lax
from jax.sharding import PartitionSpec as P


def on_device(tokens, hidden_grad, gate_value, up_value, gate_weight, up_weight):
    n_dp = lax.axis_size("dp")
    n_tp = lax.axis_size("tp")
    token_rows, features = tokens.shape
    width = gate_weight.shape[0]
    hidden_width = gate_value.shape[1]

    gate_float = gate_value.astype(jnp.float32)
    up_float = up_value.astype(jnp.float32)
    logistic = jax.nn.sigmoid(gate_float)
    upstream = hidden_grad.astype(jnp.float32)
    d_gate = (upstream * up_float * logistic * (1.0 + gate_float * (1.0 - logistic))).astype(
        jnp.bfloat16
    )
    d_up = (upstream * gate_float * logistic).astype(jnp.bfloat16)
    pieces = lax.all_gather(jnp.concatenate([d_gate, d_up], axis=1), "dp", axis=0, tiled=True)

    mine = lax.all_to_all(tokens, "dp", split_axis=1, concat_axis=0, tiled=True)
    columns = lax.all_gather(mine, "tp", axis=0, tiled=True)
    columns = columns.reshape(n_tp, n_dp, token_rows, width).transpose(1, 0, 2, 3)
    columns = columns.reshape(n_tp * n_dp * token_rows, width)

    across = (((1,), (1,)), ((), ()))
    contract = (((0,), (0,)), ((), ()))
    partial = (
        lax.dot_general(
            pieces[:, :hidden_width], gate_weight, across, preferred_element_type=jnp.float32
        )
        + lax.dot_general(
            pieces[:, hidden_width:], up_weight, across, preferred_element_type=jnp.float32
        )
    ).astype(jnp.bfloat16)
    partial = partial.reshape(n_dp, n_tp, token_rows, width).transpose(1, 0, 2, 3)
    partial = partial.reshape(n_tp * n_dp * token_rows, width)
    summed = lax.psum_scatter(partial, "tp", scatter_dimension=0, tiled=True)
    input_grad = lax.all_to_all(summed, "dp", split_axis=0, concat_axis=1, tiled=True)

    gate_grad = lax.dot_general(
        columns, pieces[:, :hidden_width], contract, preferred_element_type=jnp.float32
    ).astype(jnp.bfloat16)
    up_grad = lax.dot_general(
        columns, pieces[:, hidden_width:], contract, preferred_element_type=jnp.float32
    ).astype(jnp.bfloat16)
    return (input_grad, gate_grad, up_grad)


def solution(mesh):
    placed = (
        P(("dp", "tp"), None),
        P("dp", "tp"),
        P("dp", "tp"),
        P("dp", "tp"),
        P("dp", "tp"),
        P("dp", "tp"),
    )
    return jax.shard_map(
        on_device,
        mesh=mesh,
        in_specs=placed,
        out_specs=(P(("dp", "tp"), None), P("dp", "tp"), P("dp", "tp")),
        check_vma=False,
    )
```

```python
import functools

import jax
import jax.numpy as jnp
from jax import lax
from jax.experimental import pallas as pl
from jax.experimental.pallas import tpu as pltpu
from jax.sharding import PartitionSpec as P

MESH = pl.DeviceIdType.MESH
ACROSS = (((1,), (1,)), ((), ()))
CONTRACT = (((0,), (0,)), ((), ()))


def exchange(
    n_dp,
    n_tp,
    outer,
    inner,
    tokens_ref,
    hidden_ref,
    gate_ref,
    up_ref,
    gate_weight_hbm,
    up_weight_hbm,
    input_grad_ref,
    grads_hbm,
    columns_hbm,
    grads,
    columns,
    gate_weight,
    up_weight,
    part,
    inner_got,
    outer_send,
    outer_got,
    final,
    placed,
    local_sem,
    token_sem,
    token_outer_sem,
    token_inner_sem,
    pair_sem,
    chip_sem,
    relay_sem,
    inner_sem,
    outer_sem,
    final_sem,
    store_sem,
):
    token_rows = tokens_ref.shape[0]
    width = gate_weight.shape[0]
    hidden = gate_weight.shape[1]
    group_rows = n_tp * token_rows
    chunk_rows = inner * token_rows
    chips = n_dp // 2

    dp = lax.axis_index("dp")
    tp = lax.axis_index("tp")
    chip, core = lax.div(dp, 2), lax.rem(dp, 2)
    far, near = lax.div(tp, inner), lax.rem(tp, inner)

    def pair_device():
        return {"dp": chip * 2 + (1 - core)}

    def chip_device(offset):
        return {"dp": lax.rem(chip + offset, chips) * 2 + core}

    def dp_device(offset):
        return {"dp": lax.rem(dp + offset, n_dp)}

    def outer_device(offset):
        return {"tp": lax.rem(far + offset, outer) * inner + near}

    def inner_device(offset):
        return {"tp": far * inner + lax.rem(near + offset, inner)}

    sends = []

    def send(source, target, sems, index, device):
        copy = pltpu.make_async_remote_copy(
            src_ref=source,
            dst_ref=target,
            send_sem=sems.at[(0, *index)],
            recv_sem=sems.at[(1, *index)],
            device_id=device,
            device_id_type=MESH,
        )
        copy.start()
        sends.append(copy)
        return copy

    weight_copies = [
        pltpu.make_async_copy(gate_weight_hbm, gate_weight, local_sem.at[0]),
        pltpu.make_async_copy(up_weight_hbm, up_weight, local_sem.at[1]),
    ]
    for copy in weight_copies:
        copy.start()

    barrier = pltpu.get_barrier_semaphore()
    peers = (
        [dp_device(offset) for offset in range(1, n_dp)]
        + [outer_device(offset) for offset in range(1, outer)]
        + [inner_device(offset) for offset in range(1, inner)]
    )
    for peer in peers:
        pl.semaphore_signal(barrier, inc=1, device_id=peer, device_id_type=MESH)
    pl.semaphore_wait(barrier, len(peers))

    token_copies = []
    for offset in range(1, n_dp):
        start = pl.multiple_of(lax.rem(dp + offset, n_dp) * width, width)
        token_copies.append(
            send(
                tokens_ref.at[:, pl.ds(start, width)],
                columns.at[dp, tp],
                token_sem,
                (offset - 1,),
                dp_device(offset),
            )
        )
    own_columns = pltpu.make_async_copy(
        tokens_ref.at[:, pl.ds(pl.multiple_of(dp * width, width), width)],
        columns.at[dp, tp],
        local_sem.at[2],
    )
    own_columns.start()

    block = 256 if hidden % 256 == 0 else 128
    step_rows = 16

    def chunk_at(k):
        return lax.rem(far + k, outer)

    def rows_of(k):
        return pl.ds(pl.multiple_of(chunk_at(k) * chunk_rows, chunk_rows), chunk_rows)

    def form_chunk(k):
        base = chunk_at(k) * chunk_rows

        def form(step, carry):
            rows = pl.ds(pl.multiple_of(base + step * step_rows, step_rows), step_rows)
            for column in range(0, hidden, block):
                there = pl.ds(column, block)
                g = gate_ref[rows, there].astype(jnp.float32)
                u = up_ref[rows, there].astype(jnp.float32)
                h = hidden_ref[rows, there].astype(jnp.float32)
                s = 1.0 / (1.0 + jnp.exp(-g))
                hs = h * s
                grads[dp, rows, there] = (hs * u * (1.0 + g * (1.0 - s))).astype(jnp.bfloat16)
                grads[dp, rows, pl.ds(hidden + column, block)] = (hs * g).astype(jnp.bfloat16)
            return carry

        lax.fori_loop(0, chunk_rows // step_rows, form, 0)

    pair_copies, chip_copies = [], {}

    def send_chunk(k):
        rows = rows_of(k)
        for offset in range(1, chips):
            chip_copies[offset, k] = send(
                grads.at[dp, rows],
                grads.at[dp, rows],
                chip_sem,
                (offset - 1, k),
                chip_device(offset),
            )
        pair_copies.append(
            send(grads.at[dp, rows], grads.at[dp, rows], pair_sem, (k,), pair_device())
        )

    for k in range(outer):
        form_chunk(k)
        if k >= 1:
            send_chunk(k - 1)
    own_columns.wait()
    for copy in token_copies:
        copy.wait_recv()
    send_chunk(outer - 1)

    token_outer = [
        send(
            columns.at[:, tp],
            columns.at[:, tp],
            token_outer_sem,
            (offset - 1,),
            outer_device(offset),
        )
        for offset in range(1, outer)
    ]

    tile = 256 if width % 256 == 0 else 128

    def project(first, chunk):
        def one_tile(n, carry):
            there = pl.ds(pl.multiple_of(n * tile, tile), tile)
            if chunk is None:
                rows, count = slice(None), group_rows
            else:
                rows = pl.ds(pl.multiple_of(chunk * chunk_rows, chunk_rows), chunk_rows)
                count = chunk_rows
            d_gate = grads[pl.ds(first, 2), rows, pl.ds(0, hidden)].reshape(2 * count, hidden)
            d_up = grads[pl.ds(first, 2), rows, pl.ds(hidden, hidden)].reshape(2 * count, hidden)
            total = lax.dot_general(
                d_gate, gate_weight[there, :], ACROSS, preferred_element_type=jnp.float32
            ) + lax.dot_general(
                d_up, up_weight[there, :], ACROSS, preferred_element_type=jnp.float32
            )
            for row in range(0, 2 * count, token_rows):
                group, within = divmod(row, count)
                at, to = divmod(within // token_rows, inner)
                at = at if chunk is None else chunk
                part[first + group, at, to, :, there] = total[row : row + token_rows].astype(
                    jnp.bfloat16
                )
            return carry

        lax.fori_loop(0, width // tile, one_tile, 0)

    def send_inner(first, chip_index, k):
        at = chunk_at(k)
        return [
            send(
                part.at[pl.ds(first, 2), at, lax.rem(near + offset, inner)],
                inner_got.at[offset - 1, pl.ds(first, 2), at],
                inner_sem,
                (chip_index, k, offset - 1),
                inner_device(offset),
            )
            for offset in range(1, inner)
        ]

    outer_copies = {}

    def add_inner(first, chip_index, k, copies):
        at = chunk_at(k)
        for copy in copies:
            copy.wait_recv()
        for group in range(2):
            total = part[first + group, at, near].astype(jnp.float32)
            for offset in range(1, inner):
                total = total + inner_got[offset - 1, first + group, at].astype(jnp.float32)
            outer_send[first + group, k] = total.astype(jnp.bfloat16)
        if k > 0:
            outer_copies[chip_index, k] = send(
                outer_send.at[pl.ds(first, 2), k],
                outer_got.at[k - 1, pl.ds(first, 2)],
                outer_sem,
                (chip_index, k - 1),
                outer_device(k),
            )

    own_first = chip * 2
    for copy in pair_copies:
        copy.wait_recv()
    for copy in weight_copies:
        copy.wait()
    stores = []

    def store(source, target, index):
        copy = pltpu.make_async_copy(source, target, store_sem.at[index])
        copy.start()
        stores.append(copy)

    store(grads.at[pl.ds(own_first, 2)], grads_hbm.at[pl.ds(own_first, 2)], 0)
    project(own_first, None)
    order = list(range(1, outer)) + [0]
    own_inner = {k: send_inner(own_first, 0, k) for k in order}

    token_inner = []

    def spread_tokens(k):
        source = lax.rem(far - k + outer, outer) * inner + near
        for offset in range(1, inner):
            token_inner.append(
                send(
                    columns.at[:, source],
                    columns.at[:, source],
                    token_inner_sem,
                    (k, offset - 1),
                    inner_device(offset),
                )
            )

    spread_tokens(0)
    for k in order:
        add_inner(own_first, 0, k, own_inner[k])
    for k in range(1, outer):
        token_outer[k - 1].wait_recv()
        spread_tokens(k)

    waiting = []
    for k in range(outer):
        relays = []
        for offset in range(1, chips):
            chip_copies[offset, k].wait_recv()
            source = lax.rem(chip - offset + chips, chips) * 2 + core
            relays.append(
                send(
                    grads.at[source, rows_of(k)],
                    grads.at[source, rows_of(k)],
                    relay_sem,
                    (offset - 1, k),
                    pair_device(),
                )
            )
        for offset in range(1, chips):
            relays[offset - 1].wait_recv()
            first = lax.rem(chip - offset + chips, chips) * 2
            store(
                grads.at[pl.ds(first, 2), rows_of(k)],
                grads_hbm.at[pl.ds(first, 2), rows_of(k)],
                1 + (offset - 1) * outer + k,
            )
            project(first, chunk_at(k))
            waiting.append((first, offset, k, send_inner(first, offset, k)))
            if len(waiting) > 1:
                add_inner(*waiting.pop(0))
    while waiting:
        add_inner(*waiting.pop(0))

    for copy in token_inner:
        copy.wait_recv()
    store(columns, columns_hbm, 1 + max(chips - 1, 0) * outer)

    finals = {}
    for index in range(chips):
        first = lax.rem(chip - index + chips, chips) * 2
        for k in range(1, outer):
            outer_copies[index, k].wait_recv()
        for group in range(2):
            total = outer_send[first + group, 0].astype(jnp.float32)
            for k in range(1, outer):
                total = total + outer_got[k - 1, first + group].astype(jnp.float32)
            final[first + group] = total.astype(jnp.bfloat16)
        if index > 0:
            for turn in range(2):
                group = first + lax.rem(core + turn, 2)
                finals[index, turn] = send(
                    final.at[group],
                    placed.at[dp],
                    final_sem,
                    (index, turn),
                    {"dp": group},
                )
        else:
            finals[0, 1] = send(
                final.at[first + 1 - core], placed.at[dp], final_sem, (0, 1), pair_device()
            )
    placed[dp] = final[dp]
    for copy in finals.values():
        copy.wait_recv()
    for source in range(n_dp):
        input_grad_ref[:, source * width : (source + 1) * width] = placed[source]

    for copy in sends:
        copy.wait_send()
    for copy in stores:
        copy.wait()


def on_device(n_dp, n_tp, tokens, hidden_grad, gate_value, up_value, gate_weight, up_weight):
    token_rows, features = tokens.shape
    width, hidden = gate_weight.shape
    inner = 2 if n_tp % 2 == 0 else 1
    outer = n_tp // inner
    chips = n_dp // 2
    group_rows = n_tp * token_rows
    bf16 = jnp.bfloat16
    dma = pltpu.SemaphoreType.DMA
    vmem = pl.BlockSpec(memory_space=pltpu.VMEM)
    hbm = pl.BlockSpec(memory_space=pl.ANY)
    others = max(chips - 1, 1)
    input_grad, grads, columns = pl.pallas_call(
        functools.partial(exchange, n_dp, n_tp, outer, inner),
        out_shape=(
            jax.ShapeDtypeStruct((token_rows, features), bf16),
            jax.ShapeDtypeStruct((n_dp, group_rows, 2 * hidden), bf16),
            jax.ShapeDtypeStruct((n_dp, n_tp, token_rows, width), bf16),
        ),
        in_specs=[vmem, vmem, vmem, vmem, hbm, hbm],
        out_specs=(vmem, hbm, hbm),
        scratch_shapes=[
            pltpu.VMEM((n_dp, group_rows, 2 * hidden), bf16),
            pltpu.VMEM((n_dp, n_tp, token_rows, width), bf16),
            pltpu.VMEM((width, hidden), bf16),
            pltpu.VMEM((width, hidden), bf16),
            pltpu.VMEM((n_dp, outer, inner, token_rows, width), bf16),
            pltpu.VMEM((max(inner - 1, 1), n_dp, outer, token_rows, width), bf16),
            pltpu.VMEM((n_dp, outer, token_rows, width), bf16),
            pltpu.VMEM((max(outer - 1, 1), n_dp, token_rows, width), bf16),
            pltpu.VMEM((n_dp, token_rows, width), bf16),
            pltpu.VMEM((n_dp, token_rows, width), bf16),
            dma((3,)),
            dma((2, n_dp - 1)),
            dma((2, max(outer - 1, 1))),
            dma((2, outer, max(inner - 1, 1))),
            dma((2, outer)),
            dma((2, others, outer)),
            dma((2, others, outer)),
            dma((2, chips, outer, max(inner - 1, 1))),
            dma((2, chips, max(outer - 1, 1))),
            dma((2, chips, 2)),
            dma((2 + others * outer,)),
        ],
        compiler_params=pltpu.CompilerParams(
            collective_id=0, has_side_effects=True, vmem_limit_bytes=60 * 1024 * 1024
        ),
    )(tokens, hidden_grad, gate_value, up_value, gate_weight, up_weight)
    grads = grads.reshape(n_dp * group_rows, 2 * hidden)
    columns = columns.reshape(n_dp * group_rows, width)
    gate_grad = lax.dot_general(
        columns, grads[:, :hidden], CONTRACT, preferred_element_type=jnp.float32
    ).astype(bf16)
    up_grad = lax.dot_general(
        columns, grads[:, hidden:], CONTRACT, preferred_element_type=jnp.float32
    ).astype(bf16)
    return (input_grad, gate_grad, up_grad)


def solution(mesh):
    placed = (
        P(("dp", "tp"), None),
        P("dp", "tp"),
        P("dp", "tp"),
        P("dp", "tp"),
        P("dp", "tp"),
        P("dp", "tp"),
    )
    return jax.shard_map(
        functools.partial(on_device, mesh.shape["dp"], mesh.shape["tp"]),
        mesh=mesh,
        in_specs=placed,
        out_specs=(P(("dp", "tp"), None), P("dp", "tp"), P("dp", "tp")),
        check_vma=False,
    )
```
